32 devices in a mesh: body: 2 (over y), gx: 4 (over z), gy: 2 (over x), gz: 2 (over core).
Axes of the slice: x: 2, y: 2, z: 4, core: 2. Of those that a mesh axis runs over, the one named last changes fastest.
Arguments:
- fields: float32 [4, 3, 16, 16, 256], P('body', None, 'gx', 'gy', 'gz'), parts along dimension 0, may hold values from -0.06 to 0.06
- macro_strain: float32 [6, 3], P('body'), parts along dimension 0, may hold values from -0.15 to 0.15
- material: float32 [4], P('body'), parts along dimension 0, may hold values from 2 to 10
Outputs:
- residual: float32 [6, 16, 16, 256], P('body', 'gx', 'gy', 'gz'), parts along dimension 0
- tangent: float32 [6, 16, 16, 256], P('body', 'gx', 'gy', 'gz'), parts along dimension 0
- stats: float32 [4], P('body'), parts along dimension 0
The draws below stay inside these ranges and needn't reach their ends.
There are 2 independent parts, one for each index of `body`. The reference program is written for one: setup_inputs(seed, part) draws one part's arguments, and reference() takes and returns one part's arrays. A program takes and returns all parts, laid end to end along the dimension named above; each array names one. Nothing has to cross between parts.
All inputs are finite; a program needn't handle non-finite values.
Results may differ from the reference program's by a relative error of at most 0.0002.
Values sent between devices are 32-bit elements; how exact they have to be, the bound alone decides.
A program may use at most 64 MiB of HBM per device.

```python
import math
import jax
import jax.numpy as jnp
import numpy as np
from jax import lax

NEX = 8
NX = 16
NY = 16
NZ = 256


def draw_fields(key, part):
    bound_value = 0.06
    full_shape = (2, 3, NX, NY, NZ)
    noise_draw = jax.random.uniform(key, full_shape, jnp.float32, -1.0, 1.0)
    rising = (1.0 + 2.0 * jnp.arange(NX, dtype=jnp.float32) / (NX - 1)) / 3.0
    rising = rising[:, None, None]
    combined = noise_draw
    return (bound_value * rising * combined).astype(jnp.float32)


def setup_inputs(seed: int = 0, part: int = 0) -> dict:
    streams_of = jax.random.split(jax.random.key(seed), 4)
    part_keys = jax.random.split(jax.random.fold_in(streams_of[3], part), 4)
    fields = draw_fields(jax.random.fold_in(jax.random.fold_in(streams_of[3], part), 71), part)
    macro_strain = jnp.clip(jax.random.uniform(part_keys[1], (3, 3), jnp.float32, -0.15, 0.15), -0.15, 0.15)
    material = jnp.clip(jnp.exp(jax.random.uniform(part_keys[2], (2,), jnp.float32, math.log(2.0), math.log(10.0))), 2.0, 10.0)
    return dict(fields=fields, macro_strain=macro_strain, material=material)


highest = lax.Precision.HIGHEST
spacing = 4.0
root_eps = 1e-06

def shape_tables():
    gauss_root = math.sqrt(0.6)
    points = np.array([-gauss_root, 0.0, gauss_root])
    values = np.stack([points * (points - 1.0) / 2.0, 1.0 - points * points, points * (points + 1.0) / 2.0], axis=1)
    slopes = np.stack([points - 0.5, -2.0 * points, points + 0.5], axis=1) * (2.0 / spacing)
    weights = np.array([5.0 / 9.0, 8.0 / 9.0, 5.0 / 9.0])
    volume = weights[:, None, None] * weights[None, :, None] * weights[None, None, :] * (spacing / 2.0) ** 3
    return (jnp.asarray(values, jnp.float32), jnp.asarray(slopes, jnp.float32), jnp.asarray(volume, jnp.float32))

def triplets(array, axis, periodic):
    length = array.shape[axis]
    if periodic:
        even_nodes = lax.slice_in_dim(array, 0, length, 2, axis)
        odd_nodes = lax.slice_in_dim(array, 1, length, 2, axis)
        next_nodes = jnp.roll(even_nodes, -1, axis)
    else:
        elements = (length - 1) // 2
        even_nodes = lax.slice_in_dim(array, 0, 2 * elements, 2, axis)
        odd_nodes = lax.slice_in_dim(array, 1, 2 * elements, 2, axis)
        next_nodes = lax.slice_in_dim(array, 2, 2 * elements + 1, 2, axis)
    return jnp.stack([even_nodes, odd_nodes, next_nodes], axis=2)

def scatter_back(stacked, periodic):
    pieces = [lax.index_in_dim(stacked, slot_index, 2, keepdims=False) for slot_index in range(3)]
    if periodic:
        even_nodes = pieces[0] + jnp.roll(pieces[2], 1, axis=3)
        odd_nodes = pieces[1]
    else:
        pad_after = [(0, 0)] * pieces[0].ndim
        pad_after[3] = (0, 1)
        pad_before = [(0, 0)] * pieces[0].ndim
        pad_before[3] = (1, 0)
        even_nodes = jnp.pad(pieces[0], pad_after) + jnp.pad(pieces[2], pad_before)
        odd_nodes = jnp.pad(pieces[1], pad_after)
    paired = jnp.stack([even_nodes, odd_nodes], axis=4)
    merged_shape = paired.shape[:3] + (2 * paired.shape[3],) + paired.shape[5:]
    merged = paired.reshape(merged_shape)
    if not periodic:
        merged = lax.slice_in_dim(merged, 0, merged.shape[3] - 1, 1, 3)
    return merged

def stresses(grads, strain, shear, lame_first):
    deform = [[grads[col_at][row_at] + strain[row_at, col_at] + (1.0 if row_at == col_at else 0.0) for col_at in range(3)] for row_at in range(3)]
    change = [[grads[col_at][3 + row_at] for col_at in range(3)] for row_at in range(3)]
    cofactor = [[deform[(row_at + 1) % 3][(col_at + 1) % 3] * deform[(row_at + 2) % 3][(col_at + 2) % 3] - deform[(row_at + 1) % 3][(col_at + 2) % 3] * deform[(row_at + 2) % 3][(col_at + 1) % 3] for col_at in range(3)] for row_at in range(3)]
    volume_ratio = deform[0][0] * cofactor[0][0] + deform[0][1] * cofactor[0][1] + deform[0][2] * cofactor[0][2]
    inverse_t = [[cofactor[row_at][col_at] / volume_ratio for col_at in range(3)] for row_at in range(3)]
    log_ratio = jnp.log(volume_ratio)
    stress = [[shear * (deform[row_at][col_at] - inverse_t[row_at][col_at]) + lame_first * log_ratio * inverse_t[row_at][col_at] for col_at in range(3)] for row_at in range(3)]
    trace_term = sum((inverse_t[row_at][col_at] * change[row_at][col_at] for row_at in range(3) for col_at in range(3)))
    product = [[sum((inverse_t[row_at][mid_at] * change[col_at][mid_at] for mid_at in range(3))) for col_at in range(3)] for row_at in range(3)]
    twisted = [[sum((product[row_at][mid_at] * inverse_t[mid_at][col_at] for mid_at in range(3))) for col_at in range(3)] for row_at in range(3)]
    softening = shear - lame_first * log_ratio
    dstress = [[shear * change[row_at][col_at] + softening * twisted[row_at][col_at] + lame_first * trace_term * inverse_t[row_at][col_at] for col_at in range(3)] for row_at in range(3)]
    return (stress, dstress)

def layer_forces(slab_nodes, strain, material, periodic):
    values, slopes, volume = shape_tables()
    stacked = triplets(triplets(slab_nodes, 3, periodic), 3, periodic)
    z_value = jnp.einsum('qa,cxyaij->cxyqij', values, stacked, precision=highest)
    z_slope = jnp.einsum('qa,cxyaij->cxyqij', slopes, stacked, precision=highest)
    y_value = jnp.einsum('qa,cxazij->cxqzij', values, z_value, precision=highest)
    y_slope = jnp.einsum('qa,cxazij->cxqzij', slopes, z_value, precision=highest)
    yz_slope = jnp.einsum('qa,cxazij->cxqzij', values, z_slope, precision=highest)
    grads = [jnp.einsum('qa,cayzij->cqyzij', slopes, y_value, precision=highest), jnp.einsum('qa,cayzij->cqyzij', values, y_slope, precision=highest), jnp.einsum('qa,cayzij->cqyzij', values, yz_slope, precision=highest)]
    stress, dstress = stresses(grads, strain, material[0], material[1])
    weight = volume[:, :, :, None, None]
    fluxes = [jnp.stack([stress[0][along], stress[1][along], stress[2][along], dstress[0][along], dstress[1][along], dstress[2][along]]) * weight for along in range(3)]
    back_x0 = jnp.einsum('qa,cqyzij->cayzij', slopes, fluxes[0], precision=highest)
    back_x1 = jnp.einsum('qa,cqyzij->cayzij', values, fluxes[1], precision=highest)
    back_x2 = jnp.einsum('qa,cqyzij->cayzij', values, fluxes[2], precision=highest)
    back_y = jnp.einsum('qa,cxqzij->cxazij', values, back_x0, precision=highest) + jnp.einsum('qa,cxqzij->cxazij', slopes, back_x1, precision=highest)
    back_yz = jnp.einsum('qa,cxqzij->cxazij', values, back_x2, precision=highest)
    back_z = jnp.einsum('qa,cxyqij->cxyaij', values, back_y, precision=highest) + jnp.einsum('qa,cxyqij->cxyaij', slopes, back_yz, precision=highest)
    return scatter_back(scatter_back(back_z, periodic), periodic)

def reference(fields, macro_strain, material):
    flat = fields.reshape((6, NX, NY, NZ))
    closed = jnp.concatenate([flat, flat[:, :1]], axis=1)

    def one_layer(layer_index, accumulated):
        plane_start = (2 * layer_index).astype(jnp.int32)
        slab_nodes = lax.dynamic_slice_in_dim(closed, plane_start, 3, 1)
        contribution = layer_forces(slab_nodes, macro_strain, material, True)
        current = lax.dynamic_slice_in_dim(accumulated, plane_start, 3, 1)
        return lax.dynamic_update_slice_in_dim(accumulated, current + contribution, plane_start, 1)
    accumulated = lax.fori_loop(0, NEX, one_layer, jnp.zeros(closed.shape, jnp.float32))
    folded = jnp.concatenate([accumulated[:, :1] + accumulated[:, NX:], accumulated[:, 1:NX]], axis=1)
    residual = folded[:3]
    tangent = folded[3:]
    entries = 3.0 * NX * NY * NZ
    squares = jnp.sum(residual * residual)
    curvature = jnp.sum(flat[3:] * tangent)
    stats = jnp.stack([jnp.sqrt(squares / entries + root_eps), curvature / entries])
    return (residual, tangent, stats)
```

```python
import functools
import math

import jax
import jax.numpy as jnp
import numpy as np
from jax import lax
from jax.experimental import pallas as pl
from jax.experimental.pallas import tpu as pltpu
from jax.sharding import PartitionSpec as P

MESH = pl.DeviceIdType.MESH
BF16 = jnp.bfloat16
F32 = jnp.float32
root_eps = 1e-06
XI = math.sqrt(0.6)
HALO = 2
POINTS = np.array([-XI, 0.0, XI])
VALUES = np.stack([POINTS * (POINTS - 1) / 2, 1 - POINTS**2, POINTS * (POINTS + 1) / 2], axis=1)
SLOPES = np.stack([POINTS - 0.5, -2 * POINTS, POINTS + 0.5], axis=1) * 0.5
WEIGHTS = np.array([5 / 9, 8 / 9, 5 / 9])


def split_const(matrix):
    hi = matrix.astype(jnp.bfloat16).astype(np.float64)
    return hi, (matrix - hi).astype(jnp.bfloat16).astype(np.float64)


def stacked(matrix, depth):
    hi, lo = split_const(matrix)
    pad = np.zeros((matrix.shape[0], depth - 3 * matrix.shape[1]))
    return np.concatenate([hi, hi, lo, pad], axis=1).astype(jnp.bfloat16)


def y_tables(ny):
    elements = ny // 2 + 1
    value = np.zeros((16, 16))
    slope = np.zeros((16, 16))
    for e in range(elements):
        for a in range(3):
            node = 2 * e - 2 + a
            slot = node if 0 <= node < ny else (ny + 2 + node if node < 0 else ny + 2)
            for q in range(3):
                value[3 * e + q, slot] += VALUES[q, a]
                slope[3 * e + q, slot] += SLOPES[q, a]
    return value, slope


def forward_matrix(ny):
    value, slope = y_tables(ny)
    out = np.zeros((3, 2, 3, 16, 5, 16))
    for e in range(2):
        for q in range(3):
            for a in range(3):
                out[0, e, q, :, 2 * e + a, :] += SLOPES[q, a] * value
                out[1, e, q, :, 2 * e + a, :] += VALUES[q, a] * slope
                out[2, e, q, :, 2 * e + a, :] += VALUES[q, a] * value
    return stacked(out.reshape(288, 80), 256)


def backward_matrix(ny):
    value, slope = y_tables(ny)
    weight = np.zeros((16, 1))
    for row in range(3 * (ny // 2 + 1)):
        weight[row] = 8 * WEIGHTS[row % 3]
    out = np.zeros((2, ny, 2, 2, 16))
    for plane in range(2):
        out[plane, :, plane, 0, :] = (value * weight)[:, :ny].T
        out[plane, :, plane, 1, :] = (slope * weight)[:, :ny].T
    return stacked(out.reshape(2 * ny, 64), 256)


def stress(f, df, lame_s):
    cof = [
        [
            f[(r + 1) % 3][(c + 1) % 3] * f[(r + 2) % 3][(c + 2) % 3]
            - f[(r + 1) % 3][(c + 2) % 3] * f[(r + 2) % 3][(c + 1) % 3]
            for c in range(3)
        ]
        for r in range(3)
    ]
    jac = f[0][0] * cof[0][0] + f[0][1] * cof[0][1] + f[0][2] * cof[0][2]
    inv = 1.0 / jac
    h = [[cof[r][c] * inv for c in range(3)] for r in range(3)]
    m = lame_s * jnp.log(jac) - 1.0
    p = [[f[r][c] + m * h[r][c] for c in range(3)] for r in range(3)]
    prod = [
        [h[r][0] * df[c][0] + h[r][1] * df[c][1] + h[r][2] * df[c][2] for c in range(3)]
        for r in range(3)
    ]
    trace = lame_s * (prod[0][0] + prod[1][1] + prod[2][2])
    mix = [
        [trace - m * prod[r][c] if r == c else -(m * prod[r][c]) for c in range(3)]
        for r in range(3)
    ]
    dp = [
        [
            df[r][c] + mix[r][0] * h[0][c] + mix[r][1] * h[1][c] + mix[r][2] * h[2][c]
            for c in range(3)
        ]
        for r in range(3)
    ]
    return p, dp


def z_value(a, b):
    c = pltpu.roll(a, 127, 1)
    base = 0.4 * b + 0.3 * (a + c)
    tilt = (XI / 2) * (c - a)
    return [base - tilt, b, base + tilt]


def z_slope(a, b):
    c = pltpu.roll(a, 127, 1)
    mid = 0.25 * (c - a)
    bend = (XI / 2) * (a + c - 2.0 * b)
    return [mid - bend, mid, mid + bend]


def z_value_back(f):
    w, w0 = WEIGHTS[0], WEIGHTS[1]
    plus, minus = f[2] + f[0], f[2] - f[0]
    side = (0.3 * w) * plus
    tilt = (XI / 2 * w) * minus
    return side - tilt, (0.4 * w) * plus + w0 * f[1], side + tilt


def z_slope_back(f):
    w, w0 = WEIGHTS[0], WEIGHTS[1]
    plus, minus = f[2] + f[0], f[2] - f[0]
    mid = (0.25 * w) * plus + (0.25 * w0) * f[1]
    bend = (XI / 2 * w) * minus
    return bend - mid, -2.0 * bend, bend + mid


def hi_lo(value):
    hi = value.astype(BF16)
    return hi, (value - hi.astype(F32)).astype(BF16)


def dot(a, b):
    return jnp.dot(a, b, preferred_element_type=F32)


def stat_stages(sizes):
    if sizes[0] * sizes[1] * sizes[2] <= 32:
        return [(True, True, True)]
    return [(False, True, True), (True, False, False)]


def stage_offsets(stage, sizes):
    ranges = [range(n) if used else range(1) for used, n in zip(stage, sizes)]
    return [(a, b, c) for a in ranges[0] for b in ranges[1] for c in ranges[2] if (a, b, c) != (0, 0, 0)]


def kernel(
    sizes, strain_ref, material_ref, fields_ref, fwd_hbm, bwd_hbm,
    res_ref, tan_ref, stats_ref,
    own, main, halo, fwd, bwd, perm, perm_t, ybuf, acc, back, result, sums, partial,
    local_sem, send_sem, recv_sem, out_sem, stat_send, stat_recv,
):
    nx, ny, nz = sizes
    gx, gy, gz = lax.axis_index("gx"), lax.axis_index("gy"), lax.axis_index("gz")

    def device(ox, oy, oz):
        return {
            "gx": lax.rem(gx + ox % nx, nx),
            "gy": lax.rem(gy + oy % ny, ny),
            "gz": lax.rem(gz + oz % nz, nz),
        }

    stages = stat_stages(sizes)
    greet = {
        (ox % nx, oy % ny, oz) for ox in (-1, 0, 1) for oy in (-1, 0, 1) for oz in (0, 1)
    }
    for stage in stages:
        greet |= set(stage_offsets(stage, sizes))
    greet -= {(0, 0, 0)}
    barrier = pltpu.get_barrier_semaphore()
    for offset in sorted(greet):
        pl.semaphore_signal(barrier, inc=1, device_id=device(*offset), device_id_type=MESH)

    lanes = pl.ds(pl.multiple_of(gz * 128, 128), 128)
    get_own = pltpu.make_async_copy(fields_ref, own, local_sem.at[0])
    get_own.start()
    def keep(core):
        first, count = (2, 3) if core == 0 else (0, 4)
        return pltpu.make_async_copy(
            fields_ref.at[:, pl.ds(0, count)], main.at[:, pl.ds(first, count), :, lanes], local_sem.at[1]
        )

    for core in range(2):
        @pl.when(gz == core)
        def _():
            keep(core).start()
    get_fwd = pltpu.make_async_copy(fwd_hbm, fwd, local_sem.at[2])
    get_fwd.start()
    get_bwd = pltpu.make_async_copy(bwd_hbm, bwd, local_sem.at[3])
    get_bwd.start()

    rows = lax.broadcasted_iota(jnp.int32, (256, 256), 0)
    cols = lax.broadcasted_iota(jnp.int32, (256, 256), 1)
    perm[...] = (rows == jnp.where(cols < 128, 2 * cols, 2 * cols - 255)).astype(F32).astype(BF16)
    perm_t[...] = (cols == jnp.where(rows < 128, 2 * rows, 2 * rows - 255)).astype(F32).astype(BF16)

    get_own.wait()
    pl.semaphore_wait(barrier, len(greet))

    kinds = [(1, 0, 2, 2, 0), (-1, 1, 0, 1, 4), (0, 0, 0, 3, 2), (0, 1, 0, 4, 0)]

    def message(kind, dy, sender, target):
        _, _, plane, count, slot = kinds[kind]
        at = pl.ds(pl.multiple_of(sender * 128, 128), 128)
        side = 0 if kind < 2 else 1
        index = side * 6 + (dy + 1) * 2 + sender
        src_rows, dst = {
            0: (pl.ds(0, 8), main.at[:, pl.ds(slot, count), :, at]),
            1: (pl.ds(6, 2), halo.at[:, pl.ds(slot, count), pl.ds(0, 2), at]),
            -1: (pl.ds(0, 1), halo.at[:, pl.ds(slot, count), pl.ds(2, 1), at]),
        }[dy]
        return pltpu.make_async_remote_copy(
            src_ref=own.at[:, pl.ds(plane, count), src_rows],
            dst_ref=dst,
            send_sem=send_sem.at[kind * 3 + dy + 1],
            recv_sem=recv_sem.at[index],
            device_id=target,
            device_id_type=MESH,
        )

    def outgoing(kind, dy):
        dx, core = kinds[kind][:2]
        target = {
            "gx": lax.rem(gx + dx % nx, nx), "gy": lax.rem(gy + dy % ny, ny),
            "gz": jnp.int32(core) if core else gz * 0,
        }
        return message(kind, dy, gz, target)

    plan = [(k, dy) for k in (0, 1) for dy in (1, -1, 0)] + [(k, dy) for k in (2, 3) for dy in (1, -1)]
    for kind, dy in plan:
        outgoing(kind, dy).start()
    for core in range(2):
        @pl.when(gz == core)
        def _():
            outgoing(3 - core, 0).start()

    for core in range(2):
        @pl.when(gz == core)
        def _():
            keep(core).wait()
            me = {"gx": gx, "gy": gy, "gz": gz}
            for sender in range(2):
                for dy in (0, 1, -1):
                    if dy != 0 or sender != core:
                        message(2 + core, dy, sender, me).wait_recv()
            for sender in range(2):
                for dy in (0, 1, -1):
                    message(core, dy, sender, me).wait_recv()
    get_fwd.wait()
    get_bwd.wait()

    used = lax.broadcasted_iota(jnp.int32, (8, 256), 0) < 3
    for c in range(6):
        tiles = []
        for p in range(5):
            tiles += [main[c, p], jnp.where(used, halo[c, p], 0.0)]
        hi, lo = hi_lo(jnp.concatenate(tiles, axis=0))
        hi, lo = (dot(part, perm[...]).astype(BF16) for part in (hi, lo))
        data = jnp.concatenate([hi, lo, hi, jnp.zeros((16, 256), BF16)], axis=0)
        ybuf[c] = dot(fwd[...], data)

    shear, lame = material_ref[0], material_ref[1]
    lame_s = lame / shear
    offset = [
        [strain_ref[r, c] + (1.0 if r == c else 0.0) for c in range(3)] for r in range(3)
    ]
    for half in range(2):
        for e in range(2):
            for q in range(3):
                base = (e * 3 + q) * 16 + half * 8
                grads = []
                for c in range(6):
                    def ab(kind):
                        row = pl.ds(kind * 96 + base, 8)
                        return ybuf[c, row, 0:128], ybuf[c, row, 128:256]
                    grads.append([z_value(*ab(0)), z_value(*ab(1)), z_slope(*ab(2))])
                for qz in range(3):
                    f = [[grads[r][d][qz] + offset[r][d] for d in range(3)] for r in range(3)]
                    df = [[grads[3 + r][d][qz] for d in range(3)] for r in range(3)]
                    p, dp = stress(f, df, lame_s)
                    flux = p + dp
                    for c in range(6):
                        for plane in range(2):
                            if e == 0 and plane == 1:
                                continue
                            a = 2 if e == 0 else plane
                            for d in range(3):
                                k = float((SLOPES if d == 0 else VALUES)[q, a] * WEIGHTS[q])
                                where = (half, c, plane, d, qz)
                                first = (e == 0 and q == 0) if plane == 0 else (e == 1 and q == 0)
                                if first:
                                    acc[where] = k * flux[c][d]
                                elif k != 0.0:
                                    acc[where] += k * flux[c][d]
        for c in range(6):
            for plane in range(2):
                def at(d):
                    return [acc[half, c, plane, d, qz] for qz in range(3)]
                xa, xb, xc = z_value_back(at(0))
                ya, yb, yc = z_value_back(at(1))
                za, zb, zc = z_slope_back(at(2))
                row = pl.ds(plane * 32 + half * 8, 8)
                back[c, row, 0:128] = xa + za + pltpu.roll(xc + zc, 1, 1)
                back[c, row, 128:256] = xb + zb
                row = pl.ds(plane * 32 + 16 + half * 8, 8)
                back[c, row, 0:128] = ya + pltpu.roll(yc, 1, 1)
                back[c, row, 128:256] = yb

    nodal = []
    for c in range(6):
        hi, lo = hi_lo(back[c])
        data = jnp.concatenate([hi, lo, hi, jnp.zeros((64, 256), BF16)], axis=0)
        nodal.append(dot(bwd[...], data))
    hi, lo = hi_lo(jnp.concatenate(nodal, axis=0) * shear)
    both = dot(hi, perm_t[...]) + dot(lo, perm_t[...])
    squares = jnp.zeros((8, 256), F32)
    curvature = jnp.zeros((8, 256), F32)
    for c in range(6):
        for plane in range(2):
            value = both[c * 16 + plane * 8:c * 16 + plane * 8 + 8]
            result[c, plane] = value
            if c < 3:
                squares += value * value
            else:
                curvature += main[c, 2 + plane] * value
    partial[0:1] = jnp.sum(squares[:, :128] + squares[:, 128:], axis=0, keepdims=True)
    partial[1:2] = jnp.sum(curvature[:, :128] + curvature[:, 128:], axis=0, keepdims=True)

    pending = []
    base = 0
    for number, stage in enumerate(stages):
        offsets = stage_offsets(stage, sizes)
        sends = []
        for index, off in enumerate(offsets):
            copy = pltpu.make_async_remote_copy(
                src_ref=partial, dst_ref=sums.at[base + index],
                send_sem=stat_send.at[base + index], recv_sem=stat_recv.at[base + index],
                device_id=device(*off), device_id_type=MESH,
            )
            copy.start()
            sends.append(copy)
        if number == 0:
            planes = pl.ds(gz * 2, 2)
            other = pl.ds(pl.multiple_of((1 - gz) * 128, 128), 128)
            for n, out in enumerate((res_ref, tan_ref)):
                part = result.at[pl.ds(3 * n, 3)]
                near = pltpu.make_async_copy(part.at[:, :, :, lanes], out.at[:, planes], out_sem.at[n])
                near.start()
                far = pltpu.make_async_remote_copy(
                    src_ref=part.at[:, :, :, other], dst_ref=out.at[:, planes],
                    send_sem=out_sem.at[2 + n], recv_sem=out_sem.at[4 + n],
                    device_id=device(0, 0, 1), device_id_type=MESH,
                )
                far.start()
                pending += [near, far]
        total = partial[...]
        for copy in sends:
            copy.wait()
        for index in range(len(offsets)):
            total += sums[base + index]
        if number + 1 < len(stages):
            partial[...] = total
        base += len(offsets)

    entries = 3.0 * (4 * nx) * (8 * ny) * (128 * nz)
    whole = jnp.sum(total, axis=1, keepdims=True) * (1.0 / entries)
    whole = jnp.broadcast_to(whole, (2, 128))
    rms = jnp.sqrt(whole + root_eps)
    stats_ref[0] = rms[0, 0]
    stats_ref[1] = whole[1, 0]

    for copy in pending:
        copy.wait()
    for kind, dy in plan:
        outgoing(kind, dy).wait_send()
    for core in range(2):
        @pl.when(gz == core)
        def _():
            outgoing(3 - core, 0).wait_send()


def local(sizes, fields, macro_strain, material):
    block = fields.shape[2:]
    flat = fields.reshape((6,) + block)
    shape = jax.ShapeDtypeStruct((3,) + block, F32)
    fwd = jnp.asarray(forward_matrix(block[1]))
    bwd = jnp.asarray(backward_matrix(block[1]))
    count = sum(len(stage_offsets(stage, sizes)) for stage in stat_stages(sizes))
    vmem, dma = pltpu.VMEM, pltpu.SemaphoreType.DMA
    anywhere = pl.BlockSpec(memory_space=pl.ANY)
    smem = pl.BlockSpec(memory_space=pltpu.SMEM)
    return pl.pallas_call(
        functools.partial(kernel, sizes),
        out_shape=(shape, shape, jax.ShapeDtypeStruct((2,), F32)),
        in_specs=[smem, smem, anywhere, anywhere, anywhere],
        out_specs=(anywhere, anywhere, smem),
        scratch_shapes=[
            vmem((6,) + block, F32),
            vmem((6, 5, 8, 256), F32),
            vmem((6, 5, 8, 256), F32),
            vmem((288, 256), BF16),
            vmem((16, 256), BF16),
            vmem((256, 256), BF16),
            vmem((256, 256), BF16),
            vmem((6, 288, 256), F32),
            vmem((2, 6, 2, 3, 3, 8, 128), F32),
            vmem((6, 64, 256), F32),
            vmem((6, 2, 8, 256), F32),
            vmem((count, 2, 128), F32),
            vmem((2, 128), F32),
            dma((4,)),
            dma((12,)),
            dma((12,)),
            dma((6,)),
            dma((count,)),
            dma((count,)),
        ],
        compiler_params=pltpu.CompilerParams(collective_id=0, has_side_effects=True),
    )(macro_strain, material, flat, fwd, bwd)


def solution(mesh):
    sizes = tuple(mesh.shape[name] for name in ("gx", "gy", "gz"))
    in_specs = (P("body", None, "gx", "gy", "gz"), P("body", None), P("body"))
    out_specs = (P("body", "gx", "gy", "gz"), P("body", "gx", "gy", "gz"), P("body"))
    return jax.shard_map(
        functools.partial(local, sizes),
        mesh=mesh, in_specs=in_specs, out_specs=out_specs, check_vma=False,
    )
```

```python
import functools
import math

import jax
import jax.numpy as jnp
import numpy as np
from jax import lax
from jax.experimental import pallas as pl
from jax.experimental.pallas import tpu as pltpu
from jax.sharding import PartitionSpec as P

MESH = pl.DeviceIdType.MESH
BF16 = jnp.bfloat16
F32 = jnp.float32
root_eps = 1e-06
XI = math.sqrt(0.6)
HALO = 2
POINTS = np.array([-XI, 0.0, XI])
VALUES = np.stack([POINTS * (POINTS - 1) / 2, 1 - POINTS**2, POINTS * (POINTS + 1) / 2], axis=1)
SLOPES = np.stack([POINTS - 0.5, -2 * POINTS, POINTS + 0.5], axis=1) * 0.5
WEIGHTS = np.array([5 / 9, 8 / 9, 5 / 9])


def split_const(matrix):
    hi = matrix.astype(jnp.bfloat16).astype(np.float64)
    return hi, (matrix - hi).astype(jnp.bfloat16).astype(np.float64)


def stacked(matrix, depth):
    hi, lo = split_const(matrix)
    pad = np.zeros((matrix.shape[0], depth - 3 * matrix.shape[1]))
    return np.concatenate([hi, hi, lo, pad], axis=1).astype(jnp.bfloat16)


def y_tables(ny):
    elements = ny // 2 + 1
    value = np.zeros((16, 16))
    slope = np.zeros((16, 16))
    for e in range(elements):
        for a in range(3):
            node = 2 * e - 2 + a
            slot = node if 0 <= node < ny else (ny + 2 + node if node < 0 else ny + 2)
            for q in range(3):
                value[3 * e + q, slot] += VALUES[q, a]
                slope[3 * e + q, slot] += SLOPES[q, a]
    return value, slope


def forward_matrix(ny):
    value, slope = y_tables(ny)
    out = np.zeros((3, 3, 16, 3, 16))
    for q in range(3):
        for a in range(3):
            out[0, q, :, a, :] += SLOPES[q, a] * value
            out[1, q, :, a, :] += VALUES[q, a] * slope
            out[2, q, :, a, :] += VALUES[q, a] * value
    return stacked(out.reshape(144, 48), 256)


def backward_matrix(ny):
    value, slope = y_tables(ny)
    weight = np.zeros((16, 1))
    for row in range(3 * (ny // 2 + 1)):
        weight[row] = 8 * WEIGHTS[row % 3]
    out = np.zeros((2, ny, 2, 2, 16))
    for plane in range(2):
        out[plane, :, plane, 0, :] = (value * weight)[:, :ny].T
        out[plane, :, plane, 1, :] = (slope * weight)[:, :ny].T
    return stacked(out.reshape(2 * ny, 64), 256)


def stress(f, df, lame_s):
    cof = [
        [
            f[(r + 1) % 3][(c + 1) % 3] * f[(r + 2) % 3][(c + 2) % 3]
            - f[(r + 1) % 3][(c + 2) % 3] * f[(r + 2) % 3][(c + 1) % 3]
            for c in range(3)
        ]
        for r in range(3)
    ]
    jac = f[0][0] * cof[0][0] + f[0][1] * cof[0][1] + f[0][2] * cof[0][2]
    inv = 1.0 / jac
    h = [[cof[r][c] * inv for c in range(3)] for r in range(3)]
    m = lame_s * jnp.log(jac) - 1.0
    p = [[f[r][c] + m * h[r][c] for c in range(3)] for r in range(3)]
    prod = [
        [h[r][0] * df[c][0] + h[r][1] * df[c][1] + h[r][2] * df[c][2] for c in range(3)]
        for r in range(3)
    ]
    trace = lame_s * (prod[0][0] + prod[1][1] + prod[2][2])
    mix = [
        [trace - m * prod[r][c] if r == c else -(m * prod[r][c]) for c in range(3)]
        for r in range(3)
    ]
    dp = [
        [
            df[r][c] + mix[r][0] * h[0][c] + mix[r][1] * h[1][c] + mix[r][2] * h[2][c]
            for c in range(3)
        ]
        for r in range(3)
    ]
    return p, dp


def z_value(a, b):
    c = pltpu.roll(a, 127, 1)
    base = 0.4 * b + 0.3 * (a + c)
    tilt = (XI / 2) * (c - a)
    return [base - tilt, b, base + tilt]


def z_slope(a, b):
    c = pltpu.roll(a, 127, 1)
    mid = 0.25 * (c - a)
    bend = (XI / 2) * (a + c - 2.0 * b)
    return [mid - bend, mid, mid + bend]


def z_value_back(f):
    w, w0 = WEIGHTS[0], WEIGHTS[1]
    plus, minus = f[2] + f[0], f[2] - f[0]
    side = (0.3 * w) * plus
    tilt = (XI / 2 * w) * minus
    return side - tilt, (0.4 * w) * plus + w0 * f[1], side + tilt


def z_slope_back(f):
    w, w0 = WEIGHTS[0], WEIGHTS[1]
    plus, minus = f[2] + f[0], f[2] - f[0]
    mid = (0.25 * w) * plus + (0.25 * w0) * f[1]
    bend = (XI / 2 * w) * minus
    return bend - mid, -2.0 * bend, bend + mid


def hi_lo(value):
    hi = value.astype(BF16)
    return hi, (value - hi.astype(F32)).astype(BF16)


def dot(a, b):
    return jnp.dot(a, b, preferred_element_type=F32)


def stat_stages(sizes):
    if sizes[0] * sizes[1] * sizes[2] <= 32:
        return [(True, True, True)]
    return [(False, True, True), (True, False, False)]


def stage_offsets(stage, sizes):
    ranges = [range(n) if used else range(1) for used, n in zip(stage, sizes)]
    return [(a, b, c) for a in ranges[0] for b in ranges[1] for c in ranges[2] if (a, b, c) != (0, 0, 0)]


def kernel(
    sizes, strain_ref, material_ref, fields_ref, fwd_hbm, bwd_hbm,
    res_ref, tan_ref, stats_ref,
    own, main, halo, fwd, bwd, perm, perm_t, ybuf, acc, back, curve, result, sums, partial,
    local_sem, send_sem, recv_sem, out_sem, stat_send, stat_recv,
):
    nx, ny, nz = sizes
    gx, gy, gz = lax.axis_index("gx"), lax.axis_index("gy"), lax.axis_index("gz")

    def device(ox, oy, oz):
        return {
            "gx": lax.rem(gx + ox % nx, nx),
            "gy": lax.rem(gy + oy % ny, ny),
            "gz": lax.rem(gz + oz % nz, nz),
        }

    stages = stat_stages(sizes)
    greet = {
        (ox % nx, oy % ny, oz) for ox in (-1, 0, 1) for oy in (-1, 0, 1) for oz in (0, 1)
    }
    for stage in stages:
        greet |= set(stage_offsets(stage, sizes))
    greet -= {(0, 0, 0)}
    barrier = pltpu.get_barrier_semaphore()
    for offset in sorted(greet):
        pl.semaphore_signal(barrier, inc=1, device_id=device(*offset), device_id_type=MESH)

    lanes = pl.ds(pl.multiple_of(gz * 128, 128), 128)
    get_own = pltpu.make_async_copy(fields_ref, own, local_sem.at[0])
    get_own.start()
    def keep(core):
        first, count = (2, 3) if core == 0 else (0, 4)
        return pltpu.make_async_copy(
            fields_ref.at[:, pl.ds(0, count)], main.at[:, pl.ds(first, count), :, lanes], local_sem.at[1]
        )

    for core in range(2):
        @pl.when(gz == core)
        def _():
            keep(core).start()
    get_fwd = pltpu.make_async_copy(fwd_hbm, fwd, local_sem.at[2])
    get_fwd.start()
    get_bwd = pltpu.make_async_copy(bwd_hbm, bwd, local_sem.at[3])
    get_bwd.start()

    rows = lax.broadcasted_iota(jnp.int32, (256, 256), 0)
    cols = lax.broadcasted_iota(jnp.int32, (256, 256), 1)
    perm[...] = (rows == jnp.where(cols < 128, 2 * cols, 2 * cols - 255)).astype(F32).astype(BF16)
    perm_t[...] = (cols == jnp.where(rows < 128, 2 * rows, 2 * rows - 255)).astype(F32).astype(BF16)

    get_own.wait()
    pl.semaphore_wait(barrier, len(greet))

    kinds = [(1, 0, 2, 2, 0), (-1, 1, 0, 1, 4), (0, 0, 0, 3, 2), (0, 1, 0, 4, 0)]

    def message(kind, dy, sender, target):
        _, _, plane, count, slot = kinds[kind]
        at = pl.ds(pl.multiple_of(sender * 128, 128), 128)
        side = 0 if kind < 2 else 1
        index = side * 6 + (dy + 1) * 2 + sender
        src_rows, dst = {
            0: (pl.ds(0, 8), main.at[:, pl.ds(slot, count), :, at]),
            1: (pl.ds(6, 2), halo.at[:, pl.ds(slot, count), pl.ds(0, 2), at]),
            -1: (pl.ds(0, 1), halo.at[:, pl.ds(slot, count), pl.ds(2, 1), at]),
        }[dy]
        return pltpu.make_async_remote_copy(
            src_ref=own.at[:, pl.ds(plane, count), src_rows],
            dst_ref=dst,
            send_sem=send_sem.at[kind * 3 + dy + 1],
            recv_sem=recv_sem.at[index],
            device_id=target,
            device_id_type=MESH,
        )

    def outgoing(kind, dy):
        dx, core = kinds[kind][:2]
        target = {
            "gx": lax.rem(gx + dx % nx, nx), "gy": lax.rem(gy + dy % ny, ny),
            "gz": jnp.int32(core) if core else gz * 0,
        }
        return message(kind, dy, gz, target)

    plan = [(k, dy) for k in (0, 1) for dy in (1, -1, 0)] + [(k, dy) for k in (2, 3) for dy in (1, -1)]
    for kind, dy in plan:
        outgoing(kind, dy).start()
    for core in range(2):
        @pl.when(gz == core)
        def _():
            outgoing(3 - core, 0).start()

    get_fwd.wait()
    get_bwd.wait()
    shear, lame = material_ref[0], material_ref[1]
    lame_s = lame / shear
    offset = [
        [strain_ref[r, c] + (1.0 if r == c else 0.0) for c in range(3)] for r in range(3)
    ]
    used = lax.broadcasted_iota(jnp.int32, (8, 256), 0) < 3

    def element(e, opening):
        for c in range(6):
            tiles = []
            for p in range(2 * e, 2 * e + 3):
                tiles += [main[c, p], jnp.where(used, halo[c, p], 0.0)]
            hi, lo = hi_lo(jnp.concatenate(tiles, axis=0))
            hi, lo = (dot(part, perm[...]).astype(BF16) for part in (hi, lo))
            data = jnp.concatenate([hi, lo, hi, jnp.zeros((112, 256), BF16)], axis=0)
            ybuf[c] = dot(fwd[...], data)
        for half in range(2):
            energy = 0.0
            for q in range(3):
                base = q * 16 + half * 8
                grads = []
                for c in range(6):
                    def ab(kind):
                        row = pl.ds(kind * 48 + base, 8)
                        return ybuf[c, row, 0:128], ybuf[c, row, 128:256]
                    grads.append([z_value(*ab(0)), z_value(*ab(1)), z_slope(*ab(2))])
                for qz in range(3):
                    f = [[grads[r][d][qz] + offset[r][d] for d in range(3)] for r in range(3)]
                    df = [[grads[3 + r][d][qz] for d in range(3)] for r in range(3)]
                    p, dp = stress(f, df, lame_s)
                    flux = p + dp
                    if e == 1:
                        work = sum(dp[r][d] * df[r][d] for r in range(3) for d in range(3))
                        energy += float(8 * WEIGHTS[q] * WEIGHTS[qz]) * work
                    for c in range(6):
                        for plane in range(e + 1):
                            a = 2 if e == 0 else plane
                            for d in range(3):
                                k = float((SLOPES if d == 0 else VALUES)[q, a] * WEIGHTS[q])
                                where = (half, c, plane, d, qz)
                                if q == 0 and (opening or plane == 1):
                                    acc[where] = k * flux[c][d]
                                elif abs(k) > 1e-12:
                                    acc[where] += k * flux[c][d]
            if e == 1:
                curve[half] = energy

    for core in range(2):
        @pl.when(gz == core)
        def _():
            me = {"gx": gx, "gy": gy, "gz": gz}
            keep(core).wait()
            for sender in range(2):
                for dy in (0, 1, -1):
                    if dy != 0 or sender != core:
                        message(2 + core, dy, sender, me).wait_recv()
            element(1 - core, True)
            for sender in range(2):
                for dy in (0, 1, -1):
                    message(core, dy, sender, me).wait_recv()
            element(core, False)

    def gather(field):
        nodal = []
        for c in range(3 * field, 3 * field + 3):
            for plane in range(2):
                for half in range(2):
                    def at(d):
                        return [acc[half, c, plane, d, qz] for qz in range(3)]
                    xa, xb, xc = z_value_back(at(0))
                    ya, yb, yc = z_value_back(at(1))
                    za, zb, zc = z_slope_back(at(2))
                    row = pl.ds(plane * 32 + half * 8, 8)
                    back[c, row, 0:128] = xa + za + pltpu.roll(xc + zc, 1, 1)
                    back[c, row, 128:256] = xb + zb
                    row = pl.ds(plane * 32 + 16 + half * 8, 8)
                    back[c, row, 0:128] = ya + pltpu.roll(yc, 1, 1)
                    back[c, row, 128:256] = yb
            hi, lo = hi_lo(back[c])
            data = jnp.concatenate([hi, lo, hi, jnp.zeros((64, 256), BF16)], axis=0)
            nodal.append(dot(bwd[...], data))
        hi, lo = hi_lo(jnp.concatenate(nodal, axis=0) * shear)
        both = dot(hi, perm_t[...]) + dot(lo, perm_t[...])
        for c in range(3):
            for plane in range(2):
                result[3 * field + c, plane] = both[c * 16 + plane * 8:c * 16 + plane * 8 + 8]
        return nodal

    squares = sum(part[8 * n:8 * n + 8] * part[8 * n:8 * n + 8] for part in gather(0) for n in range(2))
    squares = (shear * shear) * (squares[:, :128] + squares[:, 128:])
    curvature = jnp.zeros((8, 128), F32)
    for half in range(2):
        point = lax.broadcasted_iota(jnp.int32, (8, 128), 0) + 8 * half
        weight = jnp.where(lax.rem(point, 3) == 1, float(WEIGHTS[1]), float(WEIGHTS[0]))
        weight = jnp.where((point >= 3) & (point < 3 * (own.shape[2] // 2 + 1)), weight, 0.0)
        curvature += weight * curve[half]
    partial[0:1] = jnp.sum(squares, axis=0, keepdims=True)
    partial[1:2] = shear * jnp.sum(curvature, axis=0, keepdims=True)

    pending = []
    base = 0
    for number, stage in enumerate(stages):
        offsets = stage_offsets(stage, sizes)
        sends = []
        for index, off in enumerate(offsets):
            copy = pltpu.make_async_remote_copy(
                src_ref=partial, dst_ref=sums.at[base + index],
                send_sem=stat_send.at[base + index], recv_sem=stat_recv.at[base + index],
                device_id=device(*off), device_id_type=MESH,
            )
            copy.start()
            sends.append(copy)
        if number == 0:
            gather(1)
            planes = pl.ds(gz * 2, 2)
            other = pl.ds(pl.multiple_of((1 - gz) * 128, 128), 128)
            for n, out in enumerate((res_ref, tan_ref)):
                part = result.at[pl.ds(3 * n, 3)]
                far = pltpu.make_async_remote_copy(
                    src_ref=part.at[:, :, :, other], dst_ref=out.at[:, planes],
                    send_sem=out_sem.at[n], recv_sem=out_sem.at[2 + n],
                    device_id=device(0, 0, 1), device_id_type=MESH,
                )
                far.start()
                pending.append(far)
                out[:, planes] = part[:, :, :, lanes]
        total = partial[...]
        for copy in sends:
            copy.wait()
        for index in range(len(offsets)):
            total += sums[base + index]
        if number + 1 < len(stages):
            partial[...] = total
        base += len(offsets)

    stats_ref[...] = total
    for copy in pending:
        copy.wait()
    for kind, dy in plan:
        outgoing(kind, dy).wait_send()
    for core in range(2):
        @pl.when(gz == core)
        def _():
            outgoing(3 - core, 0).wait_send()


def finish(entries, res, tan, total, res_ref, tan_ref, stats_ref, sem):
    copies = [pltpu.make_async_copy(res, res_ref, sem.at[0]), pltpu.make_async_copy(tan, tan_ref, sem.at[1])]
    for copy in copies:
        copy.start()
    whole = jnp.sum(total[...], axis=1, keepdims=True) * (1.0 / entries)
    whole = jnp.broadcast_to(whole, (2, 128))
    rms = jnp.sqrt(whole + root_eps)
    stats_ref[0] = rms[0, 0]
    stats_ref[1] = whole[1, 0]
    for copy in copies:
        copy.wait()


def local(sizes, fields, macro_strain, material):
    block = fields.shape[2:]
    flat = fields.reshape((6,) + block)
    shape = jax.ShapeDtypeStruct((3,) + block, F32)
    fwd = jnp.asarray(forward_matrix(block[1]))
    bwd = jnp.asarray(backward_matrix(block[1]))
    count = sum(len(stage_offsets(stage, sizes)) for stage in stat_stages(sizes))
    vmem, dma = pltpu.VMEM, pltpu.SemaphoreType.DMA
    anywhere = pl.BlockSpec(memory_space=pl.ANY)
    smem = pl.BlockSpec(memory_space=pltpu.SMEM)
    near = pl.BlockSpec(memory_space=vmem)
    res, tan, total = pl.pallas_call(
        functools.partial(kernel, sizes),
        out_shape=(vmem(shape.shape, F32), vmem(shape.shape, F32), vmem((2, 128), F32)),
        in_specs=[smem, smem, anywhere, anywhere, anywhere],
        out_specs=(near, near, near),
        scratch_shapes=[
            vmem((6,) + block, F32),
            vmem((6, 5, 8, 256), F32),
            vmem((6, 5, 8, 256), F32),
            vmem((144, 256), BF16),
            vmem((16, 256), BF16),
            vmem((256, 256), BF16),
            vmem((256, 256), BF16),
            vmem((6, 144, 256), F32),
            vmem((2, 6, 2, 3, 3, 8, 128), F32),
            vmem((6, 64, 256), F32),
            vmem((2, 8, 128), F32),
            vmem((6, 2, 8, 256), F32),
            vmem((count, 2, 128), F32),
            vmem((2, 128), F32),
            dma((4,)),
            dma((12,)),
            dma((12,)),
            dma((4,)),
            dma((count,)),
            dma((count,)),
        ],
        compiler_params=pltpu.CompilerParams(collective_id=0, has_side_effects=True),
    )(macro_strain, material, flat, fwd, bwd)
    entries = 3.0 * math.prod(n * m for n, m in zip(block, sizes))
    return pl.pallas_call(
        functools.partial(finish, entries),
        out_shape=(shape, shape, jax.ShapeDtypeStruct((2,), F32)),
        in_specs=[near, near, near],
        out_specs=(anywhere, anywhere, smem),
        scratch_shapes=[dma((2,))],
    )(*(pltpu.with_memory_space_constraint(x, vmem) for x in (res, tan, total)))


def solution(mesh):
    sizes = tuple(mesh.shape[name] for name in ("gx", "gy", "gz"))
    in_specs = (P("body", None, "gx", "gy", "gz"), P("body", None), P("body"))
    out_specs = (P("body", "gx", "gy", "gz"), P("body", "gx", "gy", "gz"), P("body"))
    return jax.shard_map(
        functools.partial(local, sizes),
        mesh=mesh, in_specs=in_specs, out_specs=out_specs, check_vma=False,
    )
```

```python
import functools
import math

import jax
import jax.numpy as jnp
import numpy as np
from jax import lax
from jax.experimental import pallas as pl
from jax.experimental.pallas import tpu as pltpu
from jax.sharding import PartitionSpec as P

MESH = pl.DeviceIdType.MESH
BF16 = jnp.bfloat16
F32 = jnp.float32
root_eps = 1e-06
XI = math.sqrt(0.6)
HALO = 2
POINTS = np.array([-XI, 0.0, XI])
VALUES = np.stack([POINTS * (POINTS - 1) / 2, 1 - POINTS**2, POINTS * (POINTS + 1) / 2], axis=1)
SLOPES = np.stack([POINTS - 0.5, -2 * POINTS, POINTS + 0.5], axis=1) * 0.5
WEIGHTS = np.array([5 / 9, 8 / 9, 5 / 9])


def split_const(matrix):
    hi = matrix.astype(jnp.bfloat16).astype(np.float64)
    return hi, (matrix - hi).astype(jnp.bfloat16).astype(np.float64)


def stacked(matrix, depth):
    hi, lo = split_const(matrix)
    pad = np.zeros((matrix.shape[0], depth - 3 * matrix.shape[1]))
    return np.concatenate([hi, hi, lo, pad], axis=1).astype(jnp.bfloat16)


def y_tables(ny):
    elements = ny // 2 + 1
    value = np.zeros((16, 16))
    slope = np.zeros((16, 16))
    for e in range(elements):
        for a in range(3):
            node = 2 * e - 2 + a
            slot = node if 0 <= node < ny else (ny + 2 + node if node < 0 else ny + 2)
            for q in range(3):
                value[3 * e + q, slot] += VALUES[q, a]
                slope[3 * e + q, slot] += SLOPES[q, a]
    return value, slope


def forward_matrix(ny):
    value, slope = y_tables(ny)
    out = np.zeros((3, 3, 16, 3, 16))
    for q in range(3):
        for a in range(3):
            out[0, q, :, a, :] += SLOPES[q, a] * value
            out[1, q, :, a, :] += VALUES[q, a] * slope
            out[2, q, :, a, :] += VALUES[q, a] * value
    return stacked(out.reshape(144, 48), 256)


def backward_matrix(ny):
    value, slope = y_tables(ny)
    weight = np.zeros((16, 1))
    for row in range(3 * (ny // 2 + 1)):
        weight[row] = 8 * WEIGHTS[row % 3]
    out = np.zeros((2, ny, 2, 2, 16))
    for plane in range(2):
        out[plane, :, plane, 0, :] = (value * weight)[:, :ny].T
        out[plane, :, plane, 1, :] = (slope * weight)[:, :ny].T
    return stacked(out.reshape(2 * ny, 64), 256)


def stress(f, df, lame_s):
    cof = [
        [
            f[(r + 1) % 3][(c + 1) % 3] * f[(r + 2) % 3][(c + 2) % 3]
            - f[(r + 1) % 3][(c + 2) % 3] * f[(r + 2) % 3][(c + 1) % 3]
            for c in range(3)
        ]
        for r in range(3)
    ]
    jac = f[0][0] * cof[0][0] + f[0][1] * cof[0][1] + f[0][2] * cof[0][2]
    inv = 1.0 / jac
    h = [[cof[r][c] * inv for c in range(3)] for r in range(3)]
    m = lame_s * jnp.log(jac) - 1.0
    p = [[f[r][c] + m * h[r][c] for c in range(3)] for r in range(3)]
    prod = [
        [h[r][0] * df[c][0] + h[r][1] * df[c][1] + h[r][2] * df[c][2] for c in range(3)]
        for r in range(3)
    ]
    trace = lame_s * (prod[0][0] + prod[1][1] + prod[2][2])
    mix = [
        [trace - m * prod[r][c] if r == c else -(m * prod[r][c]) for c in range(3)]
        for r in range(3)
    ]
    dp = [
        [
            df[r][c] + mix[r][0] * h[0][c] + mix[r][1] * h[1][c] + mix[r][2] * h[2][c]
            for c in range(3)
        ]
        for r in range(3)
    ]
    return p, dp


def z_value(a, b):
    c = pltpu.roll(a, 127, 1)
    base = 0.4 * b + 0.3 * (a + c)
    tilt = (XI / 2) * (c - a)
    return [base - tilt, b, base + tilt]


def z_slope(a, b):
    c = pltpu.roll(a, 127, 1)
    mid = 0.25 * (c - a)
    bend = (XI / 2) * (a + c - 2.0 * b)
    return [mid - bend, mid, mid + bend]


def z_value_back(f):
    w, w0 = WEIGHTS[0], WEIGHTS[1]
    plus, minus = f[2] + f[0], f[2] - f[0]
    side = (0.3 * w) * plus
    tilt = (XI / 2 * w) * minus
    return side - tilt, (0.4 * w) * plus + w0 * f[1], side + tilt


def z_slope_back(f):
    w, w0 = WEIGHTS[0], WEIGHTS[1]
    plus, minus = f[2] + f[0], f[2] - f[0]
    mid = (0.25 * w) * plus + (0.25 * w0) * f[1]
    bend = (XI / 2 * w) * minus
    return bend - mid, -2.0 * bend, bend + mid


def hi_lo(value):
    hi = value.astype(BF16)
    return hi, (value - hi.astype(F32)).astype(BF16)


def dot(a, b):
    return jnp.dot(a, b, preferred_element_type=F32)


def stat_stages(sizes):
    if sizes[0] * sizes[1] * sizes[2] <= 32:
        return [(True, True, True)]
    return [(False, True, True), (True, False, False)]


def stage_offsets(stage, sizes):
    ranges = [range(n) if used else range(1) for used, n in zip(stage, sizes)]
    return [(a, b, c) for a in ranges[0] for b in ranges[1] for c in ranges[2] if (a, b, c) != (0, 0, 0)]


def kernel(
    sizes, strain_ref, material_ref, fields_ref, fwd_hbm, bwd_hbm,
    res_ref, tan_ref, stats_ref,
    own, main, halo, fwd, bwd, perm, perm_t, ybuf, acc, back, curve, result, sums, partial,
    local_sem, send_sem, recv_sem, out_sem, stat_send, stat_recv,
):
    nx, ny, nz = sizes
    gx, gy, gz = lax.axis_index("gx"), lax.axis_index("gy"), lax.axis_index("gz")

    def device(ox, oy, oz):
        return {
            "gx": lax.rem(gx + ox % nx, nx),
            "gy": lax.rem(gy + oy % ny, ny),
            "gz": lax.rem(gz + oz % nz, nz),
        }

    stages = stat_stages(sizes)
    greet = {
        (ox % nx, oy % ny, oz) for ox in (-1, 0, 1) for oy in (-1, 0, 1) for oz in (0, 1)
    }
    for stage in stages:
        greet |= set(stage_offsets(stage, sizes))
    greet -= {(0, 0, 0)}
    barrier = pltpu.get_barrier_semaphore()
    for offset in sorted(greet):
        pl.semaphore_signal(barrier, inc=1, device_id=device(*offset), device_id_type=MESH)

    lanes = pl.ds(pl.multiple_of(gz * 128, 128), 128)
    get_own = pltpu.make_async_copy(fields_ref, own, local_sem.at[0])
    get_own.start()
    def keep(core):
        first, count = (2, 3) if core == 0 else (0, 4)
        return pltpu.make_async_copy(
            fields_ref.at[:, pl.ds(0, count)], main.at[:, pl.ds(first, count), :, lanes], local_sem.at[1]
        )

    for core in range(2):
        @pl.when(gz == core)
        def _():
            keep(core).start()
    get_fwd = pltpu.make_async_copy(fwd_hbm, fwd, local_sem.at[2])
    get_fwd.start()
    get_bwd = pltpu.make_async_copy(bwd_hbm, bwd, local_sem.at[3])
    get_bwd.start()

    rows = lax.broadcasted_iota(jnp.int32, (256, 256), 0)
    cols = lax.broadcasted_iota(jnp.int32, (256, 256), 1)
    perm[...] = (rows == jnp.where(cols < 128, 2 * cols, 2 * cols - 255)).astype(F32).astype(BF16)
    perm_t[...] = (cols == jnp.where(rows < 128, 2 * rows, 2 * rows - 255)).astype(F32).astype(BF16)

    get_own.wait()
    pl.semaphore_wait(barrier, len(greet))

    kinds = [(1, 0, 2, 2, 0), (-1, 1, 0, 1, 4), (0, 0, 0, 3, 2), (0, 1, 0, 4, 0)]

    def message(kind, dy, sender, target):
        _, _, plane, count, slot = kinds[kind]
        at = pl.ds(pl.multiple_of(sender * 128, 128), 128)
        side = 0 if kind < 2 else 1
        index = side * 6 + (dy + 1) * 2 + sender
        src_rows, dst = {
            0: (pl.ds(0, 8), main.at[:, pl.ds(slot, count), :, at]),
            1: (pl.ds(6, 2), halo.at[:, pl.ds(slot, count), pl.ds(0, 2), at]),
            -1: (pl.ds(0, 1), halo.at[:, pl.ds(slot, count), pl.ds(2, 1), at]),
        }[dy]
        return pltpu.make_async_remote_copy(
            src_ref=own.at[:, pl.ds(plane, count), src_rows],
            dst_ref=dst,
            send_sem=send_sem.at[kind * 3 + dy + 1],
            recv_sem=recv_sem.at[index],
            device_id=target,
            device_id_type=MESH,
        )

    def outgoing(kind, dy):
        dx, core = kinds[kind][:2]
        target = {
            "gx": lax.rem(gx + dx % nx, nx), "gy": lax.rem(gy + dy % ny, ny),
            "gz": jnp.int32(core) if core else gz * 0,
        }
        return message(kind, dy, gz, target)

    plan = [(k, dy) for k in (0, 1) for dy in (1, -1, 0)] + [(k, dy) for k in (2, 3) for dy in (1, -1)]
    for kind, dy in plan:
        outgoing(kind, dy).start()
    for core in range(2):
        @pl.when(gz == core)
        def _():
            outgoing(3 - core, 0).start()

    get_fwd.wait()
    get_bwd.wait()
    shear, lame = material_ref[0], material_ref[1]
    lame_s = lame / shear
    offset = [
        [strain_ref[r, c] + (1.0 if r == c else 0.0) for c in range(3)] for r in range(3)
    ]
    used = lax.broadcasted_iota(jnp.int32, (8, 256), 0) < 3

    def element(e, opening):
        tiles = []
        for c in range(6):
            for p in range(2 * e, 2 * e + 3):
                tiles += [main[c, p], jnp.where(used, halo[c, p], 0.0)]
        parts = dot(jnp.concatenate(hi_lo(jnp.concatenate(tiles, axis=0)), axis=0), perm[...]).astype(BF16)
        for c in range(6):
            hi, lo = parts[48 * c:48 * c + 48], parts[288 + 48 * c:336 + 48 * c]
            data = jnp.concatenate([hi, lo, hi, jnp.zeros((112, 256), BF16)], axis=0)
            ybuf[c] = dot(fwd[...], data)
        for half in range(2):
            energy = 0.0
            for q in range(3):
                base = q * 16 + half * 8
                grads = []
                for c in range(6):
                    def ab(kind):
                        row = pl.ds(kind * 48 + base, 8)
                        return ybuf[c, row, 0:128], ybuf[c, row, 128:256]
                    grads.append([z_value(*ab(0)), z_value(*ab(1)), z_slope(*ab(2))])
                for qz in range(3):
                    f = [[grads[r][d][qz] + offset[r][d] for d in range(3)] for r in range(3)]
                    df = [[grads[3 + r][d][qz] for d in range(3)] for r in range(3)]
                    p, dp = stress(f, df, lame_s)
                    flux = p + dp
                    if e == 1:
                        work = sum(dp[r][d] * df[r][d] for r in range(3) for d in range(3))
                        energy += float(8 * WEIGHTS[q] * WEIGHTS[qz]) * work
                    for c in range(6):
                        for plane in range(e + 1):
                            a = 2 if e == 0 else plane
                            for d in range(3):
                                k = float((SLOPES if d == 0 else VALUES)[q, a] * WEIGHTS[q])
                                where = (half, c, plane, d, qz)
                                if q == 0 and (opening or plane == 1):
                                    acc[where] = k * flux[c][d]
                                elif abs(k) > 1e-12:
                                    acc[where] += k * flux[c][d]
            if e == 1:
                curve[half] = energy

    for core in range(2):
        @pl.when(gz == core)
        def _():
            me = {"gx": gx, "gy": gy, "gz": gz}
            keep(core).wait()
            for sender in range(2):
                for dy in (0, 1, -1):
                    if dy != 0 or sender != core:
                        message(2 + core, dy, sender, me).wait_recv()
            element(1 - core, True)
            for sender in range(2):
                for dy in (0, 1, -1):
                    message(core, dy, sender, me).wait_recv()
            element(core, False)

    def gather(field):
        nodal = []
        for c in range(3 * field, 3 * field + 3):
            for plane in range(2):
                for half in range(2):
                    def at(d):
                        return [acc[half, c, plane, d, qz] for qz in range(3)]
                    xa, xb, xc = z_value_back(at(0))
                    ya, yb, yc = z_value_back(at(1))
                    za, zb, zc = z_slope_back(at(2))
                    row = pl.ds(plane * 32 + half * 8, 8)
                    back[c, row, 0:128] = xa + za + pltpu.roll(xc + zc, 1, 1)
                    back[c, row, 128:256] = xb + zb
                    row = pl.ds(plane * 32 + 16 + half * 8, 8)
                    back[c, row, 0:128] = ya + pltpu.roll(yc, 1, 1)
                    back[c, row, 128:256] = yb
            hi, lo = hi_lo(back[c])
            data = jnp.concatenate([hi, lo, hi, jnp.zeros((64, 256), BF16)], axis=0)
            nodal.append(dot(bwd[...], data))
        both = dot(jnp.concatenate(hi_lo(jnp.concatenate(nodal, axis=0) * shear), axis=0), perm_t[...])
        both = both[:48] + both[48:]
        for c in range(3):
            for plane in range(2):
                result[3 * field + c, plane] = both[c * 16 + plane * 8:c * 16 + plane * 8 + 8]
        return nodal

    squares = sum(part[8 * n:8 * n + 8] * part[8 * n:8 * n + 8] for part in gather(0) for n in range(2))
    squares = (shear * shear) * (squares[:, :128] + squares[:, 128:])
    curvature = jnp.zeros((8, 128), F32)
    for half in range(2):
        point = lax.broadcasted_iota(jnp.int32, (8, 128), 0) + 8 * half
        weight = jnp.where(lax.rem(point, 3) == 1, float(WEIGHTS[1]), float(WEIGHTS[0]))
        weight = jnp.where((point >= 3) & (point < 3 * (own.shape[2] // 2 + 1)), weight, 0.0)
        curvature += weight * curve[half]
    partial[0:1] = jnp.sum(squares, axis=0, keepdims=True)
    partial[1:2] = shear * jnp.sum(curvature, axis=0, keepdims=True)

    pending = []
    base = 0
    for number, stage in enumerate(stages):
        offsets = stage_offsets(stage, sizes)
        sends = []
        for index, off in enumerate(offsets):
            copy = pltpu.make_async_remote_copy(
                src_ref=partial, dst_ref=sums.at[base + index],
                send_sem=stat_send.at[base + index], recv_sem=stat_recv.at[base + index],
                device_id=device(*off), device_id_type=MESH,
            )
            copy.start()
            sends.append(copy)
        if number == 0:
            gather(1)
            planes = pl.ds(gz * 2, 2)
            other = pl.ds(pl.multiple_of((1 - gz) * 128, 128), 128)
            for n, out in enumerate((res_ref, tan_ref)):
                part = result.at[pl.ds(3 * n, 3)]
                far = pltpu.make_async_remote_copy(
                    src_ref=part.at[:, :, :, other], dst_ref=out.at[:, planes],
                    send_sem=out_sem.at[n], recv_sem=out_sem.at[2 + n],
                    device_id=device(0, 0, 1), device_id_type=MESH,
                )
                far.start()
                pending.append(far)
                out[:, planes] = part[:, :, :, lanes]
        total = partial[...]
        for copy in sends:
            copy.wait()
        for index in range(len(offsets)):
            total += sums[base + index]
        if number + 1 < len(stages):
            partial[...] = total
        base += len(offsets)

    stats_ref[...] = total
    for copy in pending:
        copy.wait()
    for kind, dy in plan:
        outgoing(kind, dy).wait_send()
    for core in range(2):
        @pl.when(gz == core)
        def _():
            outgoing(3 - core, 0).wait_send()


def finish(entries, res, tan, total, res_ref, tan_ref, stats_ref, sem):
    copies = [pltpu.make_async_copy(res, res_ref, sem.at[0]), pltpu.make_async_copy(tan, tan_ref, sem.at[1])]
    for copy in copies:
        copy.start()
    whole = jnp.sum(total[...], axis=1, keepdims=True) * (1.0 / entries)
    whole = jnp.broadcast_to(whole, (2, 128))
    rms = jnp.sqrt(whole + root_eps)
    stats_ref[0] = rms[0, 0]
    stats_ref[1] = whole[1, 0]
    for copy in copies:
        copy.wait()


def local(sizes, fields, macro_strain, material):
    block = fields.shape[2:]
    flat = fields.reshape((6,) + block)
    shape = jax.ShapeDtypeStruct((3,) + block, F32)
    fwd = jnp.asarray(forward_matrix(block[1]))
    bwd = jnp.asarray(backward_matrix(block[1]))
    count = sum(len(stage_offsets(stage, sizes)) for stage in stat_stages(sizes))
    vmem, dma = pltpu.VMEM, pltpu.SemaphoreType.DMA
    anywhere = pl.BlockSpec(memory_space=pl.ANY)
    smem = pl.BlockSpec(memory_space=pltpu.SMEM)
    near = pl.BlockSpec(memory_space=vmem)
    res, tan, total = pl.pallas_call(
        functools.partial(kernel, sizes),
        out_shape=(vmem(shape.shape, F32), vmem(shape.shape, F32), vmem((2, 128), F32)),
        in_specs=[smem, smem, anywhere, anywhere, anywhere],
        out_specs=(near, near, near),
        scratch_shapes=[
            vmem((6,) + block, F32),
            vmem((6, 5, 8, 256), F32),
            vmem((6, 5, 8, 256), F32),
            vmem((144, 256), BF16),
            vmem((16, 256), BF16),
            vmem((256, 256), BF16),
            vmem((256, 256), BF16),
            vmem((6, 144, 256), F32),
            vmem((2, 6, 2, 3, 3, 8, 128), F32),
            vmem((6, 64, 256), F32),
            vmem((2, 8, 128), F32),
            vmem((6, 2, 8, 256), F32),
            vmem((count, 2, 128), F32),
            vmem((2, 128), F32),
            dma((4,)),
            dma((12,)),
            dma((12,)),
            dma((4,)),
            dma((count,)),
            dma((count,)),
        ],
        compiler_params=pltpu.CompilerParams(collective_id=0, has_side_effects=True),
    )(macro_strain, material, flat, fwd, bwd)
    entries = 3.0 * math.prod(n * m for n, m in zip(block, sizes))
    return pl.pallas_call(
        functools.partial(finish, entries),
        out_shape=(shape, shape, jax.ShapeDtypeStruct((2,), F32)),
        in_specs=[near, near, near],
        out_specs=(anywhere, anywhere, smem),
        scratch_shapes=[dma((2,))],
    )(*(pltpu.with_memory_space_constraint(x, vmem) for x in (res, tan, total)))


def solution(mesh):
    sizes = tuple(mesh.shape[name] for name in ("gx", "gy", "gz"))
    in_specs = (P("body", None, "gx", "gy", "gz"), P("body", None), P("body"))
    out_specs = (P("body", "gx", "gy", "gz"), P("body", "gx", "gy", "gz"), P("body"))
    return jax.shard_map(
        functools.partial(local, sizes),
        mesh=mesh, in_specs=in_specs, out_specs=out_specs, check_vma=False,
    )
```
